32 devices in a mesh: data: 1 (over z), seq: 32 (over y, x, core).
Axes of the slice: x: 4, y: 4, z: 1, core: 2. Of those that a mesh axis runs over, the one named last changes fastest.
The devices are a block of a 4x4x8 slice.
Arguments:
- x: bfloat16 [64, 1024, 1024], P('data', 'seq')
- w_tok1: bfloat16 [2, 1024, 512], replicated
- b_tok1: float32 [2, 512], replicated
- w_tok2: bfloat16 [2, 512, 1024], replicated
- b_tok2: float32 [2, 1024], replicated
- w_ch1: bfloat16 [2, 1024, 4096], replicated
- b_ch1: float32 [2, 4096], replicated
- w_ch2: bfloat16 [2, 4096, 1024], replicated
- b_ch2: float32 [2, 1024], replicated
- ln_params: float32 [2, 4, 1024], replicated
Outputs:
- output: bfloat16 [64, 1024, 1024], P('data', 'seq')
All inputs are finite; a program needn't handle non-finite values.
Results may differ from the reference program's by a relative error of at most 0.0156138.
Values are sent between devices in bfloat16 or wider.
A program may use at most 768 MiB of HBM per device.

```python
import jax
import jax.numpy as jnp
from jax import lax

BATCH = 64
PATCHES = 1024
CHANNELS = 1024
TOKEN_HIDDEN = 512
CHANNEL_HIDDEN = 4096
LAYERS = 2
LN_EPS = 1e-6


def normal_weight(rng_key, arr_shape, fan_in, weight_gain):
    normals = jax.random.normal(rng_key, arr_shape, jnp.float32)
    return (normals * (weight_gain * fan_in ** -0.5)).astype(jnp.bfloat16)


def setup_inputs(seed: int = 0, part: int = 0) -> dict:
    key_list = jax.random.split(jax.random.key(seed), 10)
    patch_vals = jax.random.normal(jax.random.fold_in(key_list[0], part), (BATCH, PATCHES, CHANNELS), jnp.float32)
    ln_base = jnp.array([1.0, 0.0, 1.0, 0.0], jnp.float32)[None, :, None]
    return {
        "x": patch_vals.astype(jnp.bfloat16),
        "w_tok1": normal_weight(key_list[1], (LAYERS, PATCHES, TOKEN_HIDDEN), PATCHES, 1.0),
        "b_tok1": 0.5 * jax.random.normal(key_list[2], (LAYERS, TOKEN_HIDDEN), jnp.float32),
        "w_tok2": normal_weight(key_list[3], (LAYERS, TOKEN_HIDDEN, PATCHES), TOKEN_HIDDEN, 1.5),
        "b_tok2": 0.3 * jax.random.normal(key_list[4], (LAYERS, PATCHES), jnp.float32),
        "w_ch1": normal_weight(key_list[5], (LAYERS, CHANNELS, CHANNEL_HIDDEN), CHANNELS, 1.0),
        "b_ch1": 0.5 * jax.random.normal(key_list[6], (LAYERS, CHANNEL_HIDDEN), jnp.float32),
        "w_ch2": normal_weight(key_list[7], (LAYERS, CHANNEL_HIDDEN, CHANNELS), CHANNEL_HIDDEN, 1.5),
        "b_ch2": 0.3 * jax.random.normal(key_list[8], (LAYERS, CHANNELS), jnp.float32),
        "ln_params": ln_base + 0.3 * jax.random.normal(key_list[9], (LAYERS, 4, CHANNELS), jnp.float32),
    }


def layer_norm(rows_in, ln_scale, ln_offset):
    row_vals = rows_in.astype(jnp.float32)
    row_mean = jnp.mean(row_vals, axis=-1, keepdims=True)
    centered = row_vals - row_mean
    row_var = jnp.mean(centered * centered, axis=-1, keepdims=True)
    return (centered * lax.rsqrt(row_var + LN_EPS) * ln_scale + ln_offset).astype(jnp.bfloat16)


def mixer_layer(act_in, layer_params):
    w_tok1, b_tok1, w_tok2, b_tok2, w_ch1, b_ch1, w_ch2, b_ch2, ln_layer = layer_params
    u_norm = layer_norm(act_in, ln_layer[0], ln_layer[1])
    hidden = jnp.dot(w_tok1.T, u_norm, preferred_element_type=jnp.float32) + b_tok1[:, None]
    g_act = jax.nn.gelu(hidden, approximate=True).astype(jnp.bfloat16)
    t_tok = (jnp.dot(w_tok2.T, g_act, preferred_element_type=jnp.float32) + b_tok2[:, None]).astype(jnp.bfloat16)
    x_mid = (act_in.astype(jnp.float32) + t_tok.astype(jnp.float32)).astype(jnp.bfloat16)
    v_norm = layer_norm(x_mid, ln_layer[2], ln_layer[3])
    pre_act = jnp.dot(v_norm, w_ch1, preferred_element_type=jnp.float32) + b_ch1
    a_act = jax.nn.gelu(pre_act, approximate=True).astype(jnp.bfloat16)
    ch_out = jnp.dot(a_act, w_ch2, preferred_element_type=jnp.float32) + b_ch2
    return (x_mid.astype(jnp.float32) + ch_out).astype(jnp.bfloat16)


def reference(x, w_tok1, b_tok1, w_tok2, b_tok2, w_ch1, b_ch1, w_ch2, b_ch2, ln_params):
    stacked = (w_tok1, b_tok1, w_tok2, b_tok2, w_ch1, b_ch1, w_ch2, b_ch2, ln_params)

    def layer_step(state_in, layer_params):
        return mixer_layer(state_in, layer_params), None

    def one_image(image_in):
        result, _ = lax.scan(layer_step, image_in, stacked)
        return result

    return lax.map(one_image, x)
```

```python
import jax
import jax.numpy as jnp
from jax import lax
from jax.sharding import PartitionSpec as P

LN_EPS = 1e-6


def layer_norm(rows_in, ln_scale, ln_offset):
    row_vals = rows_in.astype(jnp.float32)
    row_mean = jnp.mean(row_vals, axis=-1, keepdims=True)
    centered = row_vals - row_mean
    row_var = jnp.mean(centered * centered, axis=-1, keepdims=True)
    return (centered * lax.rsqrt(row_var + LN_EPS) * ln_scale + ln_offset).astype(jnp.bfloat16)


def mixer_layer(act_in, w_tok1, b_tok1, w_tok2, b_tok2, w_ch1, b_ch1, w_ch2, b_ch2, ln_layer):
    u_norm = layer_norm(act_in, ln_layer[0], ln_layer[1])
    t_imgs = []
    for img in range(act_in.shape[0]):
        hidden = jnp.einsum("sd,sc->dc", w_tok1, u_norm[img], preferred_element_type=jnp.float32)
        g_act = jax.nn.gelu(hidden + b_tok1[:, None], approximate=True).astype(jnp.bfloat16)
        t_sum = jnp.einsum("ds,dc->sc", w_tok2, g_act, preferred_element_type=jnp.float32)
        t_imgs.append((t_sum + b_tok2[:, None]).astype(jnp.bfloat16))
    t_tok = jnp.stack(t_imgs)
    x_mid = (act_in.astype(jnp.float32) + t_tok.astype(jnp.float32)).astype(jnp.bfloat16)
    v_norm = layer_norm(x_mid, ln_layer[2], ln_layer[3])
    pre_act = jnp.einsum("bsc,ce->bse", v_norm, w_ch1, preferred_element_type=jnp.float32) + b_ch1
    a_act = jax.nn.gelu(pre_act, approximate=True).astype(jnp.bfloat16)
    ch_out = jnp.einsum("bse,ec->bsc", a_act, w_ch2, preferred_element_type=jnp.float32) + b_ch2
    return (x_mid.astype(jnp.float32) + ch_out).astype(jnp.bfloat16)


def solution(mesh):
    n = mesh.shape["seq"]

    def local_layers(x_blk, w_tok1, b_tok1, w_tok2, b_tok2, w_ch1, b_ch1, w_ch2, b_ch2, ln_params):
        images, rows, chans = x_blk.shape
        mine = images // n
        got = lax.all_to_all(x_blk, "seq", split_axis=0, concat_axis=0, tiled=True)
        act = got.reshape(n, mine, rows, chans).transpose(1, 0, 2, 3).reshape(mine, n * rows, chans)
        for k in range(w_tok1.shape[0]):
            act = mixer_layer(act, w_tok1[k], b_tok1[k], w_tok2[k], b_tok2[k], w_ch1[k], b_ch1[k], w_ch2[k], b_ch2[k], ln_params[k])
        back = act.reshape(mine, n, rows, chans).transpose(1, 0, 2, 3).reshape(n * mine, rows, chans)
        return lax.all_to_all(back, "seq", split_axis=0, concat_axis=0, tiled=True)

    act_spec = P("data", "seq", None)
    rep_spec = P()
    return jax.shard_map(local_layers, mesh=mesh, in_specs=(act_spec,) + (rep_spec,) * 9, out_specs=act_spec, check_vma=False)
```

```python
import functools

import jax
import jax.numpy as jnp
from jax import lax
from jax.experimental import pallas as pl
from jax.experimental.pallas import tpu as pltpu
from jax.sharding import PartitionSpec as P

LN_EPS = 1e-6
GELU_A = 0.7978845608028654
GELU_B = GELU_A * 0.044715
MESH = pl.DeviceIdType.MESH
BF16 = jnp.bfloat16
F32 = jnp.float32
LN_ROWS = 16


def gelu(h):
    half = 0.5 * h
    return half + half * jnp.tanh(h * (GELU_A + GELU_B * (h * h)))


def norm_rows(rows, gamma, beta):
    mean = jnp.mean(rows, axis=-1, keepdims=True)
    cent = rows - mean
    var = jnp.mean(cent * cent, axis=-1, keepdims=True)
    return (cent * lax.rsqrt(var + LN_EPS) * gamma + beta).astype(BF16)


def mixer_kernel(
    n, x_ref, wt1_ref, bt1_ref, wt2_ref, bt2_ref, wc1_ref, bc1_ref, wc2_ref, bc2_ref, ln_ref,
    out_ref, xb, w1t, w2t, s1, s2, wc1, wc2, ub, acc, ab, b1c, b2c,
    in_send, in_recv, out_send, out_recv, tok_sem, ch_sem,
):
    me = lax.axis_index("seq")
    images, rows, chans = x_ref.shape
    mine = images // n
    layers, patches, tok_hidden = wt1_ref.shape
    ch_hidden = wc1_ref.shape[2]
    blk = ub.shape[0] // 2
    blocks = patches // blk
    per_blk = n // blocks
    echunk = ab.shape[2]
    nchunk = ch_hidden // echunk

    barrier = pltpu.get_barrier_semaphore()

    def signal_peer(k, carry):
        pl.semaphore_signal(barrier, inc=1, device_id={"seq": lax.rem(me + k, n)}, device_id_type=MESH)
        return carry

    lax.fori_loop(1, n, signal_peer, 0)

    tok_copies = [pltpu.make_async_copy(wt1_ref, s1, tok_sem.at[0]), pltpu.make_async_copy(wt2_ref, s2, tok_sem.at[1])]
    for copy in tok_copies:
        copy.start()
    pl.semaphore_wait(barrier, n - 1)

    def send_in(img):
        def one(k, carry):
            peer = lax.rem(me + lax.rem(k * 11, n), n)
            pltpu.make_async_remote_copy(
                src_ref=x_ref.at[peer * mine + img],
                dst_ref=xb.at[img, pl.ds(me * rows, rows)],
                send_sem=in_send.at[img],
                recv_sem=in_recv.at[img],
                device_id={"seq": peer},
                device_id_type=MESH,
            ).start()
            return carry

        lax.fori_loop(1, n, one, 0)
        pltpu.make_async_copy(x_ref.at[me * mine + img], xb.at[img, pl.ds(me * rows, rows)], in_recv.at[img]).start()

    send_in(0)
    for k in range(layers):
        pltpu.make_async_copy(wc1_ref.at[k], wc1.at[k], ch_sem.at[0, k]).start()
        pltpu.make_async_copy(wc2_ref.at[k], wc2.at[k], ch_sem.at[1, k]).start()

    for copy in tok_copies:
        copy.wait()
    tile = 256

    def flip(k, carry):
        for r in range(0, patches, tile):
            w1t[k, :, r : r + tile] = s1[k, r : r + tile, :].T
        for r in range(0, tok_hidden, tile):
            w2t[k, :, r : r + tile] = s2[k, r : r + tile, :].T
        b1c[k] = jnp.broadcast_to(bt1_ref[pl.ds(k, 1), :], (128, tok_hidden)).T
        b2c[k] = jnp.broadcast_to(bt2_ref[pl.ds(k, 1), :], (128, patches)).T
        return carry

    lax.fori_loop(0, layers, flip, 0)

    def peer_of(b, g):
        core = g % 2
        pair = g // 2
        row = pair // 2
        parity = lax.rem(me // 2 + me // 8 + b + row, 2)
        return (pair * 2 + parity) * 2 + core

    def send_out(img, b):
        def one(g, carry):
            peer = peer_of(b, g)

            @pl.when(peer == me)
            def _():
                pltpu.make_async_copy(xb.at[img, pl.ds(peer * rows, rows)], out_ref.at[me * mine + img], out_recv.at[0]).start()

            @pl.when(peer != me)
            def _():
                pltpu.make_async_remote_copy(
                    src_ref=xb.at[img, pl.ds(peer * rows, rows)],
                    dst_ref=out_ref.at[me * mine + img],
                    send_sem=out_send.at[0],
                    recv_sem=out_recv.at[0],
                    device_id={"seq": peer},
                    device_id_type=MESH,
                ).start()

            return carry

        lax.fori_loop(0, per_blk, one, 0)

    def layer_step(step, carry):
        img = step // layers
        k = lax.rem(step, layers)

        @pl.when(k == 0)
        def _():
            pltpu.make_async_copy(xb.at[img], xb.at[img], in_recv.at[img]).wait()

        @pl.when((k == 0) & (img + 1 < mine))
        def _():
            send_in(img + 1)

        gamma1, beta1 = ln_ref[k, pl.ds(0, 1), :], ln_ref[k, pl.ds(1, 1), :]

        def ln1(r, c):
            at = pl.ds(pl.multiple_of(r * LN_ROWS, LN_ROWS), LN_ROWS)
            ub[at, :] = norm_rows(xb[img, at, :].astype(F32), gamma1, beta1)
            return c

        lax.fori_loop(0, patches // LN_ROWS, ln1, 0, unroll=4)

        half = chans // 2
        gs = []
        for c in range(0, chans, half):
            h = jnp.dot(w1t[k], ub[:, c : c + half], preferred_element_type=F32) + b1c[k, :, 0:1]
            gs.append(gelu(h).astype(BF16))
        for c, g in zip(range(0, chans, half), gs):
            t = (jnp.dot(w2t[k], g, preferred_element_type=F32) + b2c[k, :, 0:1]).astype(BF16)
            xb[img, :, c : c + half] = (xb[img, :, c : c + half].astype(F32) + t.astype(F32)).astype(BF16)

        @pl.when(img == 0)
        def _():
            pltpu.make_async_copy(wc1_ref.at[k], wc1.at[k], ch_sem.at[0, k]).wait()
            pltpu.make_async_copy(wc2_ref.at[k], wc2.at[k], ch_sem.at[1, k]).wait()

        gamma2, beta2, bias2 = ln_ref[k, pl.ds(2, 1), :], ln_ref[k, pl.ds(3, 1), :], bc2_ref[pl.ds(k, 1), :]

        def channel_block(b, c0):
            def ln2(g, c):
                at = pl.multiple_of(peer_of(b, g) * rows, rows)
                to = pl.multiple_of(g * rows, rows)
                for r in range(0, rows, LN_ROWS):
                    vals = xb[img, pl.ds(at + r, LN_ROWS), :].astype(F32)
                    ub[pl.ds(to + r, LN_ROWS), :] = norm_rows(vals, gamma2, beta2)
                    acc[pl.ds(to + r, LN_ROWS), :] = vals + bias2
                return c

            lax.fori_loop(0, per_blk, ln2, 0, unroll=2)

            def up(e, slot):
                cols = pl.ds(pl.multiple_of(e * echunk, echunk), echunk)
                h = jnp.dot(ub[0:blk, :], wc1[k, :, cols], preferred_element_type=F32) + bc1_ref[pl.ds(k, 1), cols]
                ab[slot] = gelu(h).astype(BF16)

            def down(e, slot):
                at = pl.ds(pl.multiple_of(e * echunk, echunk), echunk)
                return acc[...] + jnp.dot(ab[slot], wc2[k, at, :], preferred_element_type=F32)

            up(0, 0)

            def mid(e, c):
                acc[...] = down(e - 1, lax.rem(e - 1, 2))
                up(e, lax.rem(e, 2))
                return c

            lax.fori_loop(1, nchunk, mid, 0)
            z = down(nchunk - 1, (nchunk - 1) % 2).astype(BF16)
            for g in range(per_blk):
                at = pl.multiple_of(peer_of(b, g) * rows, rows)
                xb[img, pl.ds(at, rows), :] = z[g * rows : (g + 1) * rows]

            @pl.when(k == layers - 1)
            def _():
                send_out(img, b)

            return c0

        lax.fori_loop(0, blocks, channel_block, 0)
        return carry

    lax.fori_loop(0, mine * layers, layer_step, 0)

    for img in range(mine):
        pltpu.make_async_copy(x_ref.at[pl.ds(0, n - 1)], x_ref.at[pl.ds(0, n - 1)], in_send.at[img]).wait()
    sent = x_ref.at[pl.ds(0, mine * (n - 1))]
    pltpu.make_async_copy(sent, sent, out_send.at[0]).wait()
    pltpu.make_async_copy(out_ref, out_ref, out_recv.at[0]).wait()


def solution(mesh):
    n = mesh.shape["seq"]

    def local_layers(x_blk, w_tok1, b_tok1, w_tok2, b_tok2, w_ch1, b_ch1, w_ch2, b_ch2, ln_params):
        images, rows, chans = x_blk.shape
        mine = images // n
        layers, patches, tok_hidden = w_tok1.shape
        ch_hidden = w_ch1.shape[2]
        blk = patches // 2
        hbm = pl.BlockSpec(memory_space=pl.ANY)
        vmem = pl.BlockSpec(memory_space=pltpu.VMEM)
        flops = 4 * mine * layers * patches * chans * (tok_hidden + ch_hidden)
        dma = pltpu.SemaphoreType.DMA
        return pl.pallas_call(
            functools.partial(mixer_kernel, n),
            out_shape=jax.ShapeDtypeStruct(x_blk.shape, x_blk.dtype),
            in_specs=[hbm, hbm, vmem, hbm, vmem, hbm, vmem, hbm, vmem, vmem],
            out_specs=hbm,
            scratch_shapes=[
                pltpu.VMEM((mine, patches, chans), BF16),
                pltpu.VMEM((layers, tok_hidden, patches), BF16),
                pltpu.VMEM((layers, patches, tok_hidden), BF16),
                pltpu.VMEM((layers, patches, tok_hidden), BF16),
                pltpu.VMEM((layers, tok_hidden, patches), BF16),
                pltpu.VMEM((layers, chans, ch_hidden), BF16),
                pltpu.VMEM((layers, ch_hidden, chans), BF16),
                pltpu.VMEM((patches, chans), BF16),
                pltpu.VMEM((blk, chans), F32),
                pltpu.VMEM((2, blk, chans), BF16),
                pltpu.VMEM((layers, tok_hidden, 128), F32),
                pltpu.VMEM((layers, patches, 128), F32),
                dma((mine,)),
                dma((mine,)),
                dma((1,)),
                dma((1,)),
                dma((2,)),
                dma((2, layers)),
            ],
            compiler_params=pltpu.CompilerParams(collective_id=0, has_side_effects=True, vmem_limit_bytes=67043328),
            cost_estimate=pl.CostEstimate(flops=flops, bytes_accessed=2 * x_blk.size * 2, transcendentals=0),
        )(x_blk, w_tok1, b_tok1, w_tok2, b_tok2, w_ch1, b_ch1, w_ch2, b_ch2, ln_params)

    act_spec = P("data", "seq", None)
    rep_spec = P()
    return jax.shard_map(local_layers, mesh=mesh, in_specs=(act_spec,) + (rep_spec,) * 9, out_specs=act_spec, check_vma=False)
```

```python
import functools

import jax
import jax.numpy as jnp
from jax import lax
from jax.experimental import pallas as pl
from jax.experimental.pallas import tpu as pltpu
from jax.sharding import PartitionSpec as P

LN_EPS = 1e-6
GELU_A = 0.7978845608028654
GELU_B = GELU_A * 0.044715
MESH = pl.DeviceIdType.MESH
BF16 = jnp.bfloat16
F32 = jnp.float32
LN_ROWS = 16
UNROLL = 4
ECHUNK = 1024


def gelu(h):
    half = 0.5 * h
    return half + half * jnp.tanh(h * (GELU_A + GELU_B * (h * h)))


def norm_rows(rows, gamma, beta):
    mean = jnp.mean(rows, axis=-1, keepdims=True)
    cent = rows - mean
    var = jnp.mean(cent * cent, axis=-1, keepdims=True)
    return (cent * lax.rsqrt(var + LN_EPS) * gamma + beta).astype(BF16)


def mixer_kernel(
    n, x_ref, wt1_ref, bt1_ref, wt2_ref, bt2_ref, wc1_ref, bc1_ref, wc2_ref, bc2_ref, ln_ref,
    out_ref, state, w1t, w2t, s1, s2, wc1, wc2, ub, gb, acc, ab, b1c, b2c,
    in_send, in_recv, mid_send, mid_recv, out_sem, tok_sem, ch_sem,
):
    me = lax.axis_index("seq")
    images, rows, chans = x_ref.shape
    mine = images // n
    layers, patches, tok_hidden = wt1_ref.shape
    ch_hidden = wc1_ref.shape[2]
    halves = 2
    blk = patches // halves
    per_blk = n // halves
    echunk = ab[0].shape[1]
    nchunk = ch_hidden // echunk
    my_parity = me // 2 + me // 8
    my_place = (me // 4) * 2 + lax.rem(me, 2)

    def peer_at(b, place):
        pair = place // 2
        return pair * 4 + lax.rem(my_parity + b + pair // 2, 2) * 2 + lax.rem(place, 2)

    def turn(i):
        return lax.rem(my_place + i * 5, per_blk)

    barrier = pltpu.get_barrier_semaphore()

    def signal_peer(i, carry):
        pl.semaphore_signal(barrier, inc=1, device_id={"seq": lax.rem(me + i, n)}, device_id_type=MESH)
        return carry

    lax.fori_loop(1, n, signal_peer, 0)

    tok_copies = [pltpu.make_async_copy(wt1_ref, s1, tok_sem.at[0]), pltpu.make_async_copy(wt2_ref, s2, tok_sem.at[1])]
    for copy in tok_copies:
        copy.start()
    pl.semaphore_wait(barrier, n - 1)

    def send_in(img):
        for b in range(halves):
            def one(i, carry, b=b):
                peer = peer_at(b, turn(i))
                pltpu.make_async_remote_copy(
                    src_ref=x_ref.at[peer * mine + img],
                    dst_ref=state.at[img, pl.ds(me * rows, rows)],
                    send_sem=in_send.at[img],
                    recv_sem=in_recv.at[img, b],
                    device_id={"seq": peer},
                    device_id_type=MESH,
                ).start()
                return carry

            if b == 0:
                pltpu.make_async_copy(x_ref.at[me * mine + img], state.at[img, pl.ds(me * rows, rows)], in_recv.at[img, b]).start()
            lax.fori_loop(1 if b == 0 else 0, per_blk, one, 0)

    send_in(0)
    for k in range(layers):
        pltpu.make_async_copy(wc1_ref.at[k], wc1.at[k], ch_sem.at[0, k]).start()
        pltpu.make_async_copy(wc2_ref.at[k], wc2.at[k], ch_sem.at[1, k]).start()

    for copy in tok_copies:
        copy.wait()
    tile = 256

    def flip(k, carry):
        for r in range(0, patches, tile):
            w1t[k, :, r : r + tile] = s1[k, r : r + tile, :].T
        for r in range(0, tok_hidden, tile):
            w2t[k, :, r : r + tile] = s2[k, r : r + tile, :].T
        b1c[k] = jnp.broadcast_to(bt1_ref[pl.ds(k, 1), :], (128, tok_hidden)).T
        b2c[k] = jnp.broadcast_to(bt2_ref[pl.ds(k, 1), :], (128, patches)).T
        return carry

    lax.fori_loop(0, layers, flip, 0)

    def send_mid(img):
        for b in range(halves):
            def one(i, carry, b=b):
                peer = peer_at(b, turn(i))
                pltpu.make_async_remote_copy(
                    src_ref=state.at[img, pl.ds(peer * rows, rows)],
                    dst_ref=state.at[mine + img, pl.ds(b * blk + my_place * rows, rows)],
                    send_sem=mid_send.at[img],
                    recv_sem=mid_recv.at[img, b],
                    device_id={"seq": peer},
                    device_id_type=MESH,
                ).start()
                return carry

            if b == 0:
                state[mine + img, pl.ds(pl.multiple_of(my_place * rows, rows), rows), :] = state[img, pl.ds(pl.multiple_of(me * rows, rows), rows), :]
            lax.fori_loop(1 if b == 0 else 0, per_blk, one, 0)

    def arrived(slot, b, sem, count):
        at = state.at[slot, pl.ds(b * blk, count * rows)]
        pltpu.make_async_copy(at, at, sem).wait()

    def ln1_rows(slot, k, start):
        at = pl.ds(start, LN_ROWS)
        ub[at, :] = norm_rows(state[slot, at, :].astype(F32), ln_ref[k, pl.ds(0, 1), :], ln_ref[k, pl.ds(1, 1), :])

    def token_mix(slot, k):
        half = chans // 2
        for c in range(0, chans, half):
            h = jnp.dot(w1t[k], ub[:, c : c + half], preferred_element_type=F32) + b1c[k, :, 0:1]
            gb[:, c : c + half] = gelu(h).astype(BF16)
        for c in range(0, chans, half):
            t = (jnp.dot(w2t[k], gb[:, c : c + half], preferred_element_type=F32) + b2c[k, :, 0:1]).astype(BF16)
            state[slot, :, c : c + half] = (state[slot, :, c : c + half].astype(F32) + t.astype(F32)).astype(BF16)

    def ln2_rows(slot, k, b, r):
        vals = state[slot, pl.ds(b * blk + r, LN_ROWS), :].astype(F32)
        ub[pl.ds(b * blk + r, LN_ROWS), :] = norm_rows(vals, ln_ref[k, pl.ds(2, 1), :], ln_ref[k, pl.ds(3, 1), :])
        acc[pl.ds(r, LN_ROWS), :] = vals + bc2_ref[pl.ds(k, 1), :]

    def channel_mlp(slot, k, b):
        lo = pl.multiple_of(b * blk, blk)

        def up(e):
            cols = slice(e * echunk, (e + 1) * echunk)
            h = jnp.dot(ub[pl.ds(lo, blk), :], wc1[k, :, cols], preferred_element_type=F32) + bc1_ref[pl.ds(k, 1), cols]
            ab[e % 2][...] = gelu(h).astype(BF16)

        def down(e):
            return acc[...] + jnp.dot(ab[e % 2][...], wc2[k, e * echunk : (e + 1) * echunk, :], preferred_element_type=F32)

        up(0)
        for e in range(1, nchunk):
            up(e)
            acc[...] = down(e - 1)
        state[slot, pl.ds(lo, blk), :] = down(nchunk - 1).astype(BF16)

    def slot_step(slot, carry):
        k = slot // mine

        @pl.when(slot < mine)
        def _():
            for b in range(halves):
                arrived(slot, b, in_recv.at[slot, b], per_blk)

                def ln1(i, c, b=b):
                    start = pl.multiple_of(peer_at(b, i) * rows, rows)
                    for r in range(0, rows, LN_ROWS):
                        ln1_rows(slot, 0, start + r)
                    return c

                lax.fori_loop(0, per_blk, ln1, 0, unroll=UNROLL)

            @pl.when(slot + 1 < mine)
            def _():
                send_in(slot + 1)

            token_mix(slot, 0)

        @pl.when(lax.rem(slot, mine) == 0)
        def _():
            pltpu.make_async_copy(wc1_ref.at[k], wc1.at[k], ch_sem.at[0, k]).wait()
            pltpu.make_async_copy(wc2_ref.at[k], wc2.at[k], ch_sem.at[1, k]).wait()

        def block(b, c0):
            @pl.when((slot >= mine) & (b == 0))
            def _():
                arrived(slot, 0, mid_recv.at[slot - mine, 0], per_blk - 1)

            @pl.when((slot >= mine) & (b == 1))
            def _():
                arrived(slot, 1, mid_recv.at[slot - mine, 1], per_blk)

            def ln2(r, c):
                ln2_rows(slot, k, b, pl.multiple_of(r * LN_ROWS, LN_ROWS))
                return c

            lax.fori_loop(0, blk // LN_ROWS, ln2, 0, unroll=UNROLL)
            channel_mlp(slot, k, b)

            @pl.when(slot >= mine)
            def _():
                def one(place, c):
                    at = pl.ds(pl.multiple_of(b * blk + place * rows, rows), rows)
                    pltpu.make_async_copy(state.at[slot, at], out_ref.at[peer_at(b, place) * mine + slot - mine], out_sem.at[0]).start()
                    return c

                lax.fori_loop(0, per_blk, one, 0)

            return c0

        lax.fori_loop(0, halves, block, 0)

        @pl.when(slot < mine)
        def _():
            def ln1(r, c):
                ln1_rows(slot, 1, pl.multiple_of(r * LN_ROWS, LN_ROWS))
                return c

            lax.fori_loop(0, patches // LN_ROWS, ln1, 0, unroll=UNROLL)
            token_mix(slot, 1)
            send_mid(slot)

        return carry

    lax.fori_loop(0, mine * layers, slot_step, 0)

    sent = x_ref.at[pl.ds(0, n - 1)]
    for img in range(mine):
        pltpu.make_async_copy(sent, sent, in_send.at[img]).wait()
        pltpu.make_async_copy(sent, sent, mid_send.at[img]).wait()
    pltpu.make_async_copy(out_ref, out_ref, out_sem.at[0]).wait()


def solution(mesh):
    n = mesh.shape["seq"]

    def local_layers(x_blk, w_tok1, b_tok1, w_tok2, b_tok2, w_ch1, b_ch1, w_ch2, b_ch2, ln_params):
        images, rows, chans = x_blk.shape
        mine = images // n
        layers, patches, tok_hidden = w_tok1.shape
        ch_hidden = w_ch1.shape[2]
        blk = patches // 2
        hbm = pl.BlockSpec(memory_space=pl.ANY)
        vmem = pl.BlockSpec(memory_space=pltpu.VMEM)
        flops = 4 * mine * layers * patches * chans * (tok_hidden + ch_hidden)
        dma = pltpu.SemaphoreType.DMA
        return pl.pallas_call(
            functools.partial(mixer_kernel, n),
            out_shape=jax.ShapeDtypeStruct(x_blk.shape, x_blk.dtype),
            in_specs=[hbm, hbm, vmem, hbm, vmem, hbm, vmem, hbm, vmem, vmem],
            out_specs=hbm,
            scratch_shapes=[
                pltpu.VMEM((layers * mine, patches, chans), BF16),
                pltpu.VMEM((layers, tok_hidden, patches), BF16),
                pltpu.VMEM((layers, patches, tok_hidden), BF16),
                pltpu.VMEM((layers, patches, tok_hidden), BF16),
                pltpu.VMEM((layers, tok_hidden, patches), BF16),
                pltpu.VMEM((layers, chans, ch_hidden), BF16),
                pltpu.VMEM((layers, ch_hidden, chans), BF16),
                pltpu.VMEM((patches, chans), BF16),
                pltpu.VMEM((tok_hidden, chans), BF16),
                pltpu.VMEM((blk, chans), F32),
                [pltpu.VMEM((blk, ECHUNK), BF16)] * 2,
                pltpu.VMEM((layers, tok_hidden, 128), F32),
                pltpu.VMEM((layers, patches, 128), F32),
                dma((mine,)),
                dma((mine, 2)),
                dma((mine,)),
                dma((mine, 2)),
                dma((1,)),
                dma((2,)),
                dma((2, layers)),
            ],
            compiler_params=pltpu.CompilerParams(collective_id=0, has_side_effects=True, vmem_limit_bytes=67043328),
            cost_estimate=pl.CostEstimate(flops=flops, bytes_accessed=2 * x_blk.size * 2, transcendentals=0),
        )(x_blk, w_tok1, b_tok1, w_tok2, b_tok2, w_ch1, b_ch1, w_ch2, b_ch2, ln_params)

    act_spec = P("data", "seq", None)
    rep_spec = P()
    return jax.shard_map(local_layers, mesh=mesh, in_specs=(act_spec,) + (rep_spec,) * 9, out_specs=act_spec, check_vma=False)
```

```python
import functools

import jax
import jax.numpy as jnp
from jax import lax
from jax.experimental import pallas as pl
from jax.experimental.pallas import tpu as pltpu
from jax.sharding import PartitionSpec as P

LN_EPS = 1e-6
GELU_A = 0.7978845608028654
GELU_B = GELU_A * 0.044715
MESH = pl.DeviceIdType.MESH
BF16 = jnp.bfloat16
F32 = jnp.float32
LN_ROWS = 16
UNROLL = 16
ECHUNK = 1024


def gelu(h):
    half = 0.5 * h
    return half + half * jnp.tanh(h * (GELU_A + GELU_B * (h * h)))


def norm_rows(rows, gamma, beta):
    mean = jnp.mean(rows, axis=-1, keepdims=True)
    cent = rows - mean
    var = jnp.mean(cent * cent, axis=-1, keepdims=True)
    return (cent * lax.rsqrt(var + LN_EPS) * gamma + beta).astype(BF16)


def mixer_kernel(
    n, x_ref, wt1_ref, bt1_ref, wt2_ref, bt2_ref, wc1_ref, bc1_ref, wc2_ref, bc2_ref, ln_ref,
    out_ref, state, w1t, w2t, s1, s2, wc1, wc2, ub, vb, gb, acc, ab, b1c, b2c,
    in_send, in_recv, mid_send, mid_recv, out_sem, tok_sem, ch_sem,
):
    me = lax.axis_index("seq")
    images, rows, chans = x_ref.shape
    mine = images // n
    layers, patches, tok_hidden = wt1_ref.shape
    ch_hidden = wc1_ref.shape[2]
    halves = 2
    blk = patches // halves
    per_blk = n // halves
    echunk = ab[0].shape[1]
    nchunk = ch_hidden // echunk
    my_parity = me // 2 + me // 8
    my_place = (me // 4) * 2 + lax.rem(me, 2)

    def peer_at(b, place):
        pair = place // 2
        return pair * 4 + lax.rem(my_parity + b + pair // 2, 2) * 2 + lax.rem(place, 2)

    def turn(i):
        return lax.rem(my_place + i * 5, per_blk)

    barrier = pltpu.get_barrier_semaphore()

    def signal_peer(i, carry):
        pl.semaphore_signal(barrier, inc=1, device_id={"seq": lax.rem(me + i, n)}, device_id_type=MESH)
        return carry

    lax.fori_loop(1, n, signal_peer, 0)

    tok_copies = [pltpu.make_async_copy(wt1_ref, s1, tok_sem.at[0]), pltpu.make_async_copy(wt2_ref, s2, tok_sem.at[1])]
    for copy in tok_copies:
        copy.start()
    pl.semaphore_wait(barrier, n - 1)

    def send_in(img):
        for b in range(halves):
            def one(i, carry, b=b):
                peer = peer_at(b, turn(i))
                pltpu.make_async_remote_copy(
                    src_ref=x_ref.at[peer * mine + img],
                    dst_ref=state.at[img, pl.ds(me * rows, rows)],
                    send_sem=in_send.at[img],
                    recv_sem=in_recv.at[img, b],
                    device_id={"seq": peer},
                    device_id_type=MESH,
                ).start()
                return carry

            if b == 0:
                pltpu.make_async_copy(x_ref.at[me * mine + img], state.at[img, pl.ds(me * rows, rows)], in_recv.at[img, b]).start()
            lax.fori_loop(1 if b == 0 else 0, per_blk, one, 0)

    send_in(0)
    for k in range(layers):
        pltpu.make_async_copy(wc1_ref.at[k], wc1.at[k], ch_sem.at[0, k]).start()
        pltpu.make_async_copy(wc2_ref.at[k], wc2.at[k], ch_sem.at[1, k]).start()

    for copy in tok_copies:
        copy.wait()
    tile = 256

    def flip(k, carry):
        for r in range(0, patches, tile):
            w1t[k, :, r : r + tile] = s1[k, r : r + tile, :].T
        for r in range(0, tok_hidden, tile):
            w2t[k, :, r : r + tile] = s2[k, r : r + tile, :].T
        b1c[k] = jnp.broadcast_to(bt1_ref[pl.ds(k, 1), :], (128, tok_hidden)).T
        b2c[k] = jnp.broadcast_to(bt2_ref[pl.ds(k, 1), :], (128, patches)).T
        return carry

    lax.fori_loop(0, layers, flip, 0)

    def send_mid(img):
        for b in range(halves):
            def one(i, carry, b=b):
                peer = peer_at(b, turn(i))
                pltpu.make_async_remote_copy(
                    src_ref=state.at[img, pl.ds(peer * rows, rows)],
                    dst_ref=state.at[mine + img, pl.ds(b * blk + my_place * rows, rows)],
                    send_sem=mid_send.at[img],
                    recv_sem=mid_recv.at[img, b],
                    device_id={"seq": peer},
                    device_id_type=MESH,
                ).start()
                return carry

            if b == 0:
                state[mine + img, pl.ds(pl.multiple_of(my_place * rows, rows), rows), :] = state[img, pl.ds(pl.multiple_of(me * rows, rows), rows), :]
            lax.fori_loop(1 if b == 0 else 0, per_blk, one, 0)

    def arrived(slot, b, sem, count):
        at = state.at[slot, pl.ds(b * blk, count * rows)]
        pltpu.make_async_copy(at, at, sem).wait()

    def norm_at(dst, to, slot, start, k, which):
        vals = state[slot, pl.ds(start, LN_ROWS), :].astype(F32)
        dst[pl.ds(to, LN_ROWS), :] = norm_rows(vals, ln_ref[k, pl.ds(which, 1), :], ln_ref[k, pl.ds(which + 1, 1), :])

    def norm_block(dst, to, slot, start, k, which, count):
        def some(r, c):
            off = pl.multiple_of(r * LN_ROWS, LN_ROWS)
            norm_at(dst, to + off, slot, start + off, k, which)
            return c

        lax.fori_loop(0, count // LN_ROWS, some, 0, unroll=UNROLL)

    def token_mix(slot, k):
        half = chans // 2
        for c in range(0, chans, half):
            h = jnp.dot(w1t[k], ub[:, c : c + half], preferred_element_type=F32) + b1c[k, :, 0:1]
            gb[:, c : c + half] = gelu(h).astype(BF16)
        for c in range(0, chans, half):
            t = (jnp.dot(w2t[k], gb[:, c : c + half], preferred_element_type=F32) + b2c[k, :, 0:1]).astype(BF16)
            state[slot, :, c : c + half] = (state[slot, :, c : c + half].astype(F32) + t.astype(F32)).astype(BF16)

    def channel_mlp(slot, k, b):
        lo = pl.multiple_of(b * blk, blk)
        other = jnp.where((slot == mine * layers - 1) | (b == 1), 0, 1) * blk
        side_k = jnp.minimum(k + b, layers - 1)
        side_which = 2 * (1 - b)
        side_rows = blk // nchunk

        def side(e):
            for r in range(e * side_rows, (e + 1) * side_rows, LN_ROWS):
                norm_at(ub, r, slot, pl.multiple_of(other, blk) + r, side_k, side_which)

        def up(e):
            cols = slice(e * echunk, (e + 1) * echunk)
            h = jnp.dot(vb[...], wc1[k, :, cols], preferred_element_type=F32) + bc1_ref[pl.ds(k, 1), cols]
            ab[e % 2][...] = gelu(h).astype(BF16)

        def down(e):
            base = state[slot, pl.ds(lo, blk), :].astype(F32) + bc2_ref[pl.ds(k, 1), :] if e == 0 else acc[...]
            return base + jnp.dot(ab[e % 2][...], wc2[k, e * echunk : (e + 1) * echunk, :], preferred_element_type=F32)

        up(0)
        side(0)
        for e in range(1, nchunk):
            up(e)
            side(e)
            acc[...] = down(e - 1)
        state[slot, pl.ds(lo, blk), :] = down(nchunk - 1).astype(BF16)

    def slot_step(slot, carry):
        k = slot // mine

        @pl.when(slot < mine)
        def _():
            for b in range(halves):
                arrived(slot, b, in_recv.at[slot, b], per_blk)

                def ln1(i, c, b=b):
                    start = pl.multiple_of(peer_at(b, i) * rows, rows)
                    for r in range(0, rows, LN_ROWS):
                        norm_at(ub, start + r, slot, start + r, 0, 0)
                    return c

                lax.fori_loop(0, per_blk, ln1, 0, unroll=min(UNROLL, per_blk))

            @pl.when(slot + 1 < mine)
            def _():
                send_in(slot + 1)

            token_mix(slot, 0)

        @pl.when(lax.rem(slot, mine) == 0)
        def _():
            pltpu.make_async_copy(wc1_ref.at[k], wc1.at[k], ch_sem.at[0, k]).wait()
            pltpu.make_async_copy(wc2_ref.at[k], wc2.at[k], ch_sem.at[1, k]).wait()

        last = mine * layers - 1

        def block(b, c0):
            fresh = (b == 0) | (slot == last)

            @pl.when((slot >= mine) & (b == 0))
            def _():
                arrived(slot, 0, mid_recv.at[slot - mine, 0], per_blk - 1)

            @pl.when((slot >= mine) & ((b == 1) == (slot == last)))
            def _():
                arrived(slot, 1, mid_recv.at[slot - mine, 1], per_blk)

            @pl.when(fresh)
            def _():
                norm_block(vb, 0, slot, pl.multiple_of(b * blk, blk), k, 2, blk)

            @pl.when(jnp.logical_not(fresh))
            def _():
                vb[...] = ub[0:blk, :]

            channel_mlp(slot, k, b)

            @pl.when(slot >= mine)
            def _():
                def one(place, c):
                    at = pl.ds(pl.multiple_of(b * blk + place * rows, rows), rows)
                    pltpu.make_async_copy(state.at[slot, at], out_ref.at[peer_at(b, place) * mine + slot - mine], out_sem.at[0]).start()
                    return c

                lax.fori_loop(0, per_blk, one, 0)

            return c0

        lax.fori_loop(0, halves, block, 0)

        @pl.when(slot < mine)
        def _():
            norm_block(ub, blk, slot, blk, 1, 0, blk)
            token_mix(slot, 1)
            send_mid(slot)

        return carry

    lax.fori_loop(0, mine * layers, slot_step, 0)

    sent = x_ref.at[pl.ds(0, n - 1)]
    for img in range(mine):
        pltpu.make_async_copy(sent, sent, in_send.at[img]).wait()
        pltpu.make_async_copy(sent, sent, mid_send.at[img]).wait()
    pltpu.make_async_copy(out_ref, out_ref, out_sem.at[0]).wait()


def solution(mesh):
    n = mesh.shape["seq"]

    def local_layers(x_blk, w_tok1, b_tok1, w_tok2, b_tok2, w_ch1, b_ch1, w_ch2, b_ch2, ln_params):
        images, rows, chans = x_blk.shape
        mine = images // n
        layers, patches, tok_hidden = w_tok1.shape
        ch_hidden = w_ch1.shape[2]
        blk = patches // 2
        hbm = pl.BlockSpec(memory_space=pl.ANY)
        vmem = pl.BlockSpec(memory_space=pltpu.VMEM)
        flops = 4 * mine * layers * patches * chans * (tok_hidden + ch_hidden)
        dma = pltpu.SemaphoreType.DMA
        return pl.pallas_call(
            functools.partial(mixer_kernel, n),
            out_shape=jax.ShapeDtypeStruct(x_blk.shape, x_blk.dtype),
            in_specs=[hbm, hbm, vmem, hbm, vmem, hbm, vmem, hbm, vmem, vmem],
            out_specs=hbm,
            scratch_shapes=[
                pltpu.VMEM((layers * mine, patches, chans), BF16),
                pltpu.VMEM((layers, tok_hidden, patches), BF16),
                pltpu.VMEM((layers, patches, tok_hidden), BF16),
                pltpu.VMEM((layers, patches, tok_hidden), BF16),
                pltpu.VMEM((layers, tok_hidden, patches), BF16),
                pltpu.VMEM((layers, chans, ch_hidden), BF16),
                pltpu.VMEM((layers, ch_hidden, chans), BF16),
                pltpu.VMEM((patches, chans), BF16),
                pltpu.VMEM((blk, chans), BF16),
                pltpu.VMEM((tok_hidden, chans), BF16),
                pltpu.VMEM((blk, chans), F32),
                [pltpu.VMEM((blk, ECHUNK), BF16)] * 2,
                pltpu.VMEM((layers, tok_hidden, 128), F32),
                pltpu.VMEM((layers, patches, 128), F32),
                dma((mine,)),
                dma((mine, 2)),
                dma((mine,)),
                dma((mine, 2)),
                dma((1,)),
                dma((2,)),
                dma((2, layers)),
            ],
            compiler_params=pltpu.CompilerParams(collective_id=0, has_side_effects=True, vmem_limit_bytes=67043328),
            cost_estimate=pl.CostEstimate(flops=flops, bytes_accessed=2 * x_blk.size * 2, transcendentals=0),
        )(x_blk, w_tok1, b_tok1, w_tok2, b_tok2, w_ch1, b_ch1, w_ch2, b_ch2, ln_params)

    act_spec = P("data", "seq", None)
    rep_spec = P()
    return jax.shard_map(local_layers, mesh=mesh, in_specs=(act_spec,) + (rep_spec,) * 9, out_specs=act_spec, check_vma=False)
```

```python
import functools

import jax
import jax.numpy as jnp
from jax import lax
from jax.experimental import pallas as pl
from jax.experimental.pallas import tpu as pltpu
from jax.sharding import PartitionSpec as P

LN_EPS = 1e-6
GELU_A = 0.7978845608028654
GELU_B = GELU_A * 0.044715
MESH = pl.DeviceIdType.MESH
BF16 = jnp.bfloat16
F32 = jnp.float32
LN_ROWS = 16
UNROLL = 16
SENDS = 8
ECHUNK = 1024


def gelu(h):
    half = 0.5 * h
    return half + half * jnp.tanh(h * (GELU_A + GELU_B * (h * h)))


def norm_rows(rows, gamma, beta):
    mean = jnp.mean(rows, axis=-1, keepdims=True)
    cent = rows - mean
    var = jnp.mean(cent * cent, axis=-1, keepdims=True)
    return (cent * lax.rsqrt(var + LN_EPS) * gamma + beta).astype(BF16)


def mixer_kernel(
    n, x_ref, wt1_ref, bt1_hbm, wt2_ref, bt2_hbm, wc1_ref, bc1_hbm, wc2_ref, bc2_hbm, ln_hbm,
    out_ref, state, bt1_ref, bt2_ref, bc1_ref, bc2_ref, ln_ref, w1t, w2t, s1, s2, wc1, wc2, ub, vb, gb, acc, ab, b1c, b2c,
    in_send, in_recv, mid_send, mid_recv, tok_sem, ch_sem, small_sem,
):
    me = lax.axis_index("seq")
    images, rows, chans = x_ref.shape
    mine = images // n
    layers, patches, tok_hidden = wt1_ref.shape
    ch_hidden = wc1_ref.shape[2]
    halves = 2
    blk = patches // halves
    per_blk = n // halves
    echunk = ab[0].shape[1]
    nchunk = ch_hidden // echunk
    my_parity = me // 2 + me // 8
    my_place = (me // 4) * 2 + lax.rem(me, 2)

    def peer_at(b, place):
        pair = place // 2
        return pair * 4 + lax.rem(my_parity + b + pair // 2, 2) * 2 + lax.rem(place, 2)

    def turn(i):
        return lax.rem(my_place + i * 5, per_blk)

    def stage(k):
        return pltpu.make_async_copy(wt1_ref.at[k], s1, tok_sem.at[0]), pltpu.make_async_copy(wt2_ref.at[k], s2, tok_sem.at[1])

    smalls = [
        pltpu.make_async_copy(src, dst, small_sem.at[i])
        for i, (src, dst) in enumerate(
            ((bt1_hbm, bt1_ref), (bt2_hbm, bt2_ref), (bc1_hbm, bc1_ref), (bc2_hbm, bc2_ref), (ln_hbm, ln_ref))
        )
    ]

    barrier = pltpu.get_barrier_semaphore()

    def signal_peer(i, carry):
        pl.semaphore_signal(barrier, inc=1, device_id={"seq": lax.rem(me + i, n)}, device_id_type=MESH)
        return carry

    lax.fori_loop(1, n, signal_peer, 0, unroll=SENDS)

    for copy in (*stage(0), *smalls):
        copy.start()
    pl.semaphore_wait(barrier, n - 1)

    def send_in(img):
        for b in range(halves):
            def one(i, carry, b=b):
                peer = peer_at(b, turn(i))
                pltpu.make_async_remote_copy(
                    src_ref=x_ref.at[peer * mine + img],
                    dst_ref=state.at[img, pl.ds(me * rows, rows)],
                    send_sem=in_send.at[img],
                    recv_sem=in_recv.at[img, b],
                    device_id={"seq": peer},
                    device_id_type=MESH,
                ).start()
                return carry

            if b == 0:
                pltpu.make_async_copy(x_ref.at[me * mine + img], state.at[img, pl.ds(me * rows, rows)], in_recv.at[img, b]).start()
            lax.fori_loop(1 if b == 0 else 0, per_blk, one, 0, unroll=SENDS)

    send_in(0)
    for k in range(layers):
        pltpu.make_async_copy(wc1_ref.at[k], wc1.at[k], ch_sem.at[0, k]).start()
        pltpu.make_async_copy(wc2_ref.at[k], wc2.at[k], ch_sem.at[1, k]).start()

    for copy in smalls:
        copy.wait()
    tile = 256

    def flip(k, carry):
        for copy in stage(k):
            copy.wait()
        for r in range(0, patches, tile):
            w1t[k, :, r : r + tile] = s1[r : r + tile, :].T
        for r in range(0, tok_hidden, tile):
            w2t[k, :, r : r + tile] = s2[r : r + tile, :].T

        @pl.when(k + 1 < layers)
        def _():
            for copy in stage(k + 1):
                copy.start()

        b1c[k] = jnp.broadcast_to(bt1_ref[pl.ds(k, 1), :], (128, tok_hidden)).T
        b2c[k] = jnp.broadcast_to(bt2_ref[pl.ds(k, 1), :], (128, patches)).T
        return carry

    lax.fori_loop(0, layers, flip, 0)

    def send_mid(img):
        for b in range(halves):
            def one(i, carry, b=b):
                peer = peer_at(b, turn(i))
                pltpu.make_async_remote_copy(
                    src_ref=state.at[img, pl.ds(peer * rows, rows)],
                    dst_ref=state.at[mine + img, pl.ds(b * blk + my_place * rows, rows)],
                    send_sem=mid_send.at[img],
                    recv_sem=mid_recv.at[img, b],
                    device_id={"seq": peer},
                    device_id_type=MESH,
                ).start()
                return carry

            if b == 0:
                state[mine + img, pl.ds(pl.multiple_of(my_place * rows, rows), rows), :] = state[img, pl.ds(pl.multiple_of(me * rows, rows), rows), :]
            lax.fori_loop(1 if b == 0 else 0, per_blk, one, 0, unroll=SENDS)

    def arrived(slot, b, sem, count):
        at = state.at[slot, pl.ds(b * blk, count * rows)]
        pltpu.make_async_copy(at, at, sem).wait()

    def norm_at(dst, to, slot, start, k, which):
        vals = state[slot, pl.ds(start, LN_ROWS), :].astype(F32)
        dst[pl.ds(to, LN_ROWS), :] = norm_rows(vals, ln_ref[k, pl.ds(which, 1), :], ln_ref[k, pl.ds(which + 1, 1), :])

    def norm_block(dst, to, slot, start, k, which, count):
        def some(r, c):
            off = pl.multiple_of(r * LN_ROWS, LN_ROWS)
            norm_at(dst, to + off, slot, start + off, k, which)
            return c

        lax.fori_loop(0, count // LN_ROWS, some, 0, unroll=UNROLL)

    def token_mix(slot, k):
        half = chans // 2
        for c in range(0, chans, half):
            h = jnp.dot(w1t[k], ub[:, c : c + half], preferred_element_type=F32) + b1c[k, :, 0:1]
            gb[:, c : c + half] = gelu(h).astype(BF16)
        for c in range(0, chans, half):
            t = (jnp.dot(w2t[k], gb[:, c : c + half], preferred_element_type=F32) + b2c[k, :, 0:1]).astype(BF16)
            state[slot, :, c : c + half] = (state[slot, :, c : c + half].astype(F32) + t.astype(F32)).astype(BF16)

    def channel_mlp(slot, k, b):
        lo = pl.multiple_of(b * blk, blk)
        other = jnp.where((slot == mine * layers - 1) | (b == 1), 0, 1) * blk
        side_k = jnp.minimum(k + b, layers - 1)
        side_which = 2 * (1 - b)
        side_rows = blk // nchunk

        def side(e):
            for r in range(e * side_rows, (e + 1) * side_rows, LN_ROWS):
                norm_at(ub, r, slot, pl.multiple_of(other, blk) + r, side_k, side_which)

        def up(e):
            cols = slice(e * echunk, (e + 1) * echunk)
            h = jnp.dot(vb[...], wc1[k, :, cols], preferred_element_type=F32) + bc1_ref[pl.ds(k, 1), cols]
            ab[e % 2][...] = gelu(h).astype(BF16)

        def down(e):
            base = state[slot, pl.ds(lo, blk), :].astype(F32) + bc2_ref[pl.ds(k, 1), :] if e == 0 else acc[...]
            return base + jnp.dot(ab[e % 2][...], wc2[k, e * echunk : (e + 1) * echunk, :], preferred_element_type=F32)

        up(0)
        side(0)
        for e in range(1, nchunk):
            up(e)
            side(e)
            acc[...] = down(e - 1)
        state[slot, pl.ds(lo, blk), :] = down(nchunk - 1).astype(BF16)

    def slot_step(slot, carry):
        k = slot // mine

        @pl.when(slot < mine)
        def _():
            for b in range(halves):
                arrived(slot, b, in_recv.at[slot, b], per_blk)

                def ln1(i, c, b=b):
                    start = pl.multiple_of(peer_at(b, i) * rows, rows)
                    for r in range(0, rows, LN_ROWS):
                        norm_at(ub, start + r, slot, start + r, 0, 0)
                    return c

                lax.fori_loop(0, per_blk, ln1, 0, unroll=min(UNROLL, per_blk))

            @pl.when(slot + 1 < mine)
            def _():
                send_in(slot + 1)

            token_mix(slot, 0)

        @pl.when(lax.rem(slot, mine) == 0)
        def _():
            pltpu.make_async_copy(wc1_ref.at[k], wc1.at[k], ch_sem.at[0, k]).wait()
            pltpu.make_async_copy(wc2_ref.at[k], wc2.at[k], ch_sem.at[1, k]).wait()

        last = mine * layers - 1

        def block(b, c0):
            fresh = (b == 0) | (slot == last)

            @pl.when((slot >= mine) & (b == 0))
            def _():
                arrived(slot, 0, mid_recv.at[slot - mine, 0], per_blk - 1)

            @pl.when((slot >= mine) & ((b == 1) == (slot == last)))
            def _():
                arrived(slot, 1, mid_recv.at[slot - mine, 1], per_blk)

            @pl.when(fresh)
            def _():
                norm_block(vb, 0, slot, pl.multiple_of(b * blk, blk), k, 2, blk)

            @pl.when(jnp.logical_not(fresh))
            def _():
                vb[...] = ub[0:blk, :]

            channel_mlp(slot, k, b)

            @pl.when(slot >= mine)
            def _():
                def one(place, c):
                    at = pl.ds(pl.multiple_of(b * blk + place * rows, rows), rows)
                    out_ref[peer_at(b, place) * mine + slot - mine] = state[slot, at, :]
                    return c

                lax.fori_loop(0, per_blk, one, 0, unroll=4)

            return c0

        lax.fori_loop(0, halves, block, 0)

        @pl.when(slot < mine)
        def _():
            norm_block(ub, blk, slot, blk, 1, 0, blk)
            token_mix(slot, 1)
            send_mid(slot)

        return carry

    lax.fori_loop(0, mine * layers, slot_step, 0)

    sent = x_ref.at[pl.ds(0, n - 1)]
    for img in range(mine):
        pltpu.make_async_copy(sent, sent, in_send.at[img]).wait()
        pltpu.make_async_copy(sent, sent, mid_send.at[img]).wait()


def solution(mesh):
    n = mesh.shape["seq"]

    def local_layers(x_blk, w_tok1, b_tok1, w_tok2, b_tok2, w_ch1, b_ch1, w_ch2, b_ch2, ln_params):
        images, rows, chans = x_blk.shape
        mine = images // n
        layers, patches, tok_hidden = w_tok1.shape
        ch_hidden = w_ch1.shape[2]
        blk = patches // 2
        hbm = pl.BlockSpec(memory_space=pl.ANY)
        vmem = pl.BlockSpec(memory_space=pltpu.VMEM)
        flops = 4 * mine * layers * patches * chans * (tok_hidden + ch_hidden)
        dma = pltpu.SemaphoreType.DMA
        return pl.pallas_call(
            functools.partial(mixer_kernel, n),
            out_shape=pltpu.VMEM(x_blk.shape, x_blk.dtype),
            in_specs=[hbm] * 10,
            out_specs=vmem,
            scratch_shapes=[
                pltpu.VMEM((layers * mine, patches, chans), BF16),
                pltpu.VMEM(b_tok1.shape, F32),
                pltpu.VMEM(b_tok2.shape, F32),
                pltpu.VMEM(b_ch1.shape, F32),
                pltpu.VMEM(b_ch2.shape, F32),
                pltpu.VMEM(ln_params.shape, F32),
                pltpu.VMEM((layers, tok_hidden, patches), BF16),
                pltpu.VMEM((layers, patches, tok_hidden), BF16),
                pltpu.VMEM((patches, tok_hidden), BF16),
                pltpu.VMEM((tok_hidden, patches), BF16),
                pltpu.VMEM((layers, chans, ch_hidden), BF16),
                pltpu.VMEM((layers, ch_hidden, chans), BF16),
                pltpu.VMEM((patches, chans), BF16),
                pltpu.VMEM((blk, chans), BF16),
                pltpu.VMEM((tok_hidden, chans), BF16),
                pltpu.VMEM((blk, chans), F32),
                [pltpu.VMEM((blk, ECHUNK), BF16)] * 2,
                pltpu.VMEM((layers, tok_hidden, 128), F32),
                pltpu.VMEM((layers, patches, 128), F32),
                dma((mine,)),
                dma((mine, 2)),
                dma((mine,)),
                dma((mine, 2)),
                dma((2,)),
                dma((2, layers)),
                dma((5,)),
            ],
            compiler_params=pltpu.CompilerParams(collective_id=0, has_side_effects=True, vmem_limit_bytes=62783488),
            cost_estimate=pl.CostEstimate(flops=flops, bytes_accessed=2 * x_blk.size * 2, transcendentals=0),
        )(x_blk, w_tok1, b_tok1, w_tok2, b_tok2, w_ch1, b_ch1, w_ch2, b_ch2, ln_params)

    act_spec = P("data", "seq", None)
    rep_spec = P()
    return jax.shard_map(local_layers, mesh=mesh, in_specs=(act_spec,) + (rep_spec,) * 9, out_specs=act_spec, check_vma=False)
```

```python
import functools

import jax
import jax.numpy as jnp
from jax import lax
from jax.experimental import pallas as pl
from jax.experimental.pallas import tpu as pltpu
from jax.sharding import PartitionSpec as P

LN_EPS = 1e-6
GELU_A = 0.7978845608028654
GELU_B = GELU_A * 0.044715
MESH = pl.DeviceIdType.MESH
BF16 = jnp.bfloat16
F32 = jnp.float32
LN_ROWS = 16
UNROLL = 16
SENDS = 8
ECHUNK = 1024


def gelu_twice(h):
    return h + h * jnp.tanh(h * (2 * GELU_A + 8 * GELU_B * (h * h)))


def norm_rows(rows, gamma, beta):
    mean = jnp.mean(rows, axis=-1, keepdims=True)
    cent = rows - mean
    var = jnp.mean(cent * cent, axis=-1, keepdims=True)
    return (cent * lax.rsqrt(var + LN_EPS) * gamma + beta).astype(BF16)


def mixer_kernel(
    n, x_ref, wt1_ref, bt1_hbm, wt2_ref, bt2_hbm, wc1_ref, bc1_hbm, wc2_ref, bc2_hbm, ln_hbm,
    out_ref, state, bt1_ref, bt2_ref, bc1_ref, bc2_ref, ln_ref, w1t, w2t, s1, s2, wc1, wc2, ub, vb, gb, acc, ab, b1c, b2c,
    in_send, in_recv, mid_send, mid_recv, tok_sem, ch_sem, small_sem,
):
    me = lax.axis_index("seq")
    images, rows, chans = x_ref.shape
    mine = images // n
    layers, patches, tok_hidden = wt1_ref.shape
    ch_hidden = wc1_ref.shape[2]
    halves = 2
    blk = patches // halves
    per_blk = n // halves
    echunk = ab[0].shape[1]
    nchunk = ch_hidden // echunk
    my_parity = me // 2 + me // 8
    my_place = (me // 4) * 2 + lax.rem(me, 2)

    def peer_at(b, place):
        pair = place // 2
        return pair * 4 + lax.rem(my_parity + b + pair // 2, 2) * 2 + lax.rem(place, 2)

    def turn(i):
        return lax.rem(my_place + i * 5, per_blk)

    def stage(k):
        return pltpu.make_async_copy(wt1_ref.at[k], s1, tok_sem.at[0]), pltpu.make_async_copy(wt2_ref.at[k], s2, tok_sem.at[1])

    smalls = [
        pltpu.make_async_copy(src, dst, small_sem.at[i])
        for i, (src, dst) in enumerate(
            ((bt1_hbm, bt1_ref), (bt2_hbm, bt2_ref), (bc1_hbm, bc1_ref), (bc2_hbm, bc2_ref), (ln_hbm, ln_ref))
        )
    ]

    barrier = pltpu.get_barrier_semaphore()

    def signal_peer(i, carry):
        pl.semaphore_signal(barrier, inc=1, device_id={"seq": lax.rem(me + i, n)}, device_id_type=MESH)
        return carry

    lax.fori_loop(1, n, signal_peer, 0, unroll=SENDS)

    for copy in (*stage(0), *smalls):
        copy.start()
    pl.semaphore_wait(barrier, n - 1)

    def send_in(img):
        for b in range(halves):
            def one(i, carry, b=b):
                peer = peer_at(b, turn(i))
                pltpu.make_async_remote_copy(
                    src_ref=x_ref.at[peer * mine + img],
                    dst_ref=state.at[img, pl.ds(me * rows, rows)],
                    send_sem=in_send.at[img],
                    recv_sem=in_recv.at[img, b],
                    device_id={"seq": peer},
                    device_id_type=MESH,
                ).start()
                return carry

            if b == 0:
                pltpu.make_async_copy(x_ref.at[me * mine + img], state.at[img, pl.ds(me * rows, rows)], in_recv.at[img, b]).start()
            lax.fori_loop(1 if b == 0 else 0, per_blk, one, 0, unroll=SENDS)

    send_in(0)
    for k in range(layers):
        pltpu.make_async_copy(wc1_ref.at[k], wc1.at[k], ch_sem.at[0, k]).start()
        pltpu.make_async_copy(wc2_ref.at[k], wc2.at[k], ch_sem.at[1, k]).start()

    for copy in smalls:
        copy.wait()
    tile = 256

    def flip(k, carry):
        for copy in stage(k):
            copy.wait()
        for r in range(0, patches, tile):
            w1t[k, :, r : r + tile] = s1[r : r + tile, :].T
        for r in range(0, tok_hidden, tile):
            w2t[k, :, r : r + tile] = s2[r : r + tile, :].T

        @pl.when(k + 1 < layers)
        def _():
            for copy in stage(k + 1):
                copy.start()

        b1c[k] = jnp.broadcast_to(0.5 * bt1_ref[pl.ds(k, 1), :], (128, tok_hidden)).T
        b2c[k] = jnp.broadcast_to(bt2_ref[pl.ds(k, 1), :], (128, patches)).T
        return carry

    lax.fori_loop(0, layers, flip, 0)

    def send_mid(img):
        for b in range(halves):
            def one(i, carry, b=b):
                peer = peer_at(b, turn(i))
                pltpu.make_async_remote_copy(
                    src_ref=state.at[img, pl.ds(peer * rows, rows)],
                    dst_ref=state.at[mine + img, pl.ds(b * blk + my_place * rows, rows)],
                    send_sem=mid_send.at[img],
                    recv_sem=mid_recv.at[img, b],
                    device_id={"seq": peer},
                    device_id_type=MESH,
                ).start()
                return carry

            if b == 0:
                state[mine + img, pl.ds(pl.multiple_of(my_place * rows, rows), rows), :] = state[img, pl.ds(pl.multiple_of(me * rows, rows), rows), :]
            lax.fori_loop(1 if b == 0 else 0, per_blk, one, 0, unroll=SENDS)

    def arrived(slot, b, sem, count):
        at = state.at[slot, pl.ds(b * blk, count * rows)]
        pltpu.make_async_copy(at, at, sem).wait()

    def norm_at(dst, to, slot, start, k, which):
        vals = state[slot, pl.ds(start, LN_ROWS), :].astype(F32)
        dst[pl.ds(to, LN_ROWS), :] = norm_rows(vals, 0.5 * ln_ref[k, pl.ds(which, 1), :], 0.5 * ln_ref[k, pl.ds(which + 1, 1), :])

    def norm_block(dst, to, slot, start, k, which, count):
        def some(r, c):
            off = pl.multiple_of(r * LN_ROWS, LN_ROWS)
            norm_at(dst, to + off, slot, start + off, k, which)
            return c

        lax.fori_loop(0, count // LN_ROWS, some, 0, unroll=UNROLL)

    def token_mix(slot, k):
        half = chans // 2
        for c in range(0, chans, half):
            h = jnp.dot(w1t[k], ub[:, c : c + half], preferred_element_type=F32) + b1c[k, :, 0:1]
            gb[:, c : c + half] = gelu_twice(h).astype(BF16)
        for c in range(0, chans, half):
            t = (jnp.dot(w2t[k], gb[:, c : c + half], preferred_element_type=F32) + b2c[k, :, 0:1]).astype(BF16)
            state[slot, :, c : c + half] = (state[slot, :, c : c + half].astype(F32) + t.astype(F32)).astype(BF16)

    def channel_mlp(slot, k, b):
        lo = pl.multiple_of(b * blk, blk)
        other = jnp.where((slot == mine * layers - 1) | (b == 1), 0, 1) * blk
        side_k = jnp.minimum(k + b, layers - 1)
        side_which = 2 * (1 - b)
        side_rows = blk // nchunk

        def side(e):
            for r in range(e * side_rows, (e + 1) * side_rows, LN_ROWS):
                norm_at(ub, r, slot, pl.multiple_of(other, blk) + r, side_k, side_which)

        def up(e):
            cols = slice(e * echunk, (e + 1) * echunk)
            h = jnp.dot(vb[...], wc1[k, :, cols], preferred_element_type=F32) + 0.5 * bc1_ref[pl.ds(k, 1), cols]
            ab[e % 2][...] = gelu_twice(h).astype(BF16)

        def down(e):
            base = state[slot, pl.ds(lo, blk), :].astype(F32) + bc2_ref[pl.ds(k, 1), :] if e == 0 else acc[...]
            return base + jnp.dot(ab[e % 2][...], wc2[k, e * echunk : (e + 1) * echunk, :], preferred_element_type=F32)

        up(0)
        side(0)
        for e in range(1, nchunk):
            up(e)
            side(e)
            acc[...] = down(e - 1)
        state[slot, pl.ds(lo, blk), :] = down(nchunk - 1).astype(BF16)

    def slot_step(slot, carry):
        k = slot // mine

        @pl.when(slot < mine)
        def _():
            for b in range(halves):
                arrived(slot, b, in_recv.at[slot, b], per_blk)

                if b == 0:
                    @pl.when(slot + 1 < mine)
                    def _():
                        send_in(slot + 1)

                def ln1(i, c, b=b):
                    start = pl.multiple_of(peer_at(b, i) * rows, rows)
                    for r in range(0, rows, LN_ROWS):
                        norm_at(ub, start + r, slot, start + r, 0, 0)
                    return c

                lax.fori_loop(0, per_blk, ln1, 0, unroll=min(UNROLL, per_blk))

            token_mix(slot, 0)

        @pl.when(lax.rem(slot, mine) == 0)
        def _():
            pltpu.make_async_copy(wc1_ref.at[k], wc1.at[k], ch_sem.at[0, k]).wait()
            pltpu.make_async_copy(wc2_ref.at[k], wc2.at[k], ch_sem.at[1, k]).wait()

        last = mine * layers - 1

        def block(b, c0):
            fresh = (b == 0) | (slot == last)

            @pl.when((slot >= mine) & (b == 0))
            def _():
                arrived(slot, 0, mid_recv.at[slot - mine, 0], per_blk - 1)

            @pl.when((slot >= mine) & ((b == 1) == (slot == last)))
            def _():
                arrived(slot, 1, mid_recv.at[slot - mine, 1], per_blk)

            @pl.when(fresh)
            def _():
                norm_block(vb, 0, slot, pl.multiple_of(b * blk, blk), k, 2, blk)

            @pl.when(jnp.logical_not(fresh))
            def _():
                vb[...] = ub[0:blk, :]

            channel_mlp(slot, k, b)

            @pl.when(slot >= mine)
            def _():
                def one(place, c):
                    at = pl.ds(pl.multiple_of(b * blk + place * rows, rows), rows)
                    out_ref[peer_at(b, place) * mine + slot - mine] = state[slot, at, :]
                    return c

                lax.fori_loop(0, per_blk, one, 0, unroll=4)

            return c0

        lax.fori_loop(0, halves, block, 0)

        @pl.when(slot < mine)
        def _():
            for r in range(blk, patches, LN_ROWS):
                norm_at(ub, r, slot, r, 1, 0)
            token_mix(slot, 1)
            send_mid(slot)

        return carry

    lax.fori_loop(0, mine * layers, slot_step, 0)

    sent = x_ref.at[pl.ds(0, n - 1)]
    for img in range(mine):
        pltpu.make_async_copy(sent, sent, in_send.at[img]).wait()
        pltpu.make_async_copy(sent, sent, mid_send.at[img]).wait()


def solution(mesh):
    n = mesh.shape["seq"]

    def local_layers(x_blk, w_tok1, b_tok1, w_tok2, b_tok2, w_ch1, b_ch1, w_ch2, b_ch2, ln_params):
        images, rows, chans = x_blk.shape
        mine = images // n
        layers, patches, tok_hidden = w_tok1.shape
        ch_hidden = w_ch1.shape[2]
        blk = patches // 2
        hbm = pl.BlockSpec(memory_space=pl.ANY)
        vmem = pl.BlockSpec(memory_space=pltpu.VMEM)
        flops = 4 * mine * layers * patches * chans * (tok_hidden + ch_hidden)
        dma = pltpu.SemaphoreType.DMA
        return pl.pallas_call(
            functools.partial(mixer_kernel, n),
            out_shape=pltpu.VMEM(x_blk.shape, x_blk.dtype),
            in_specs=[hbm] * 10,
            out_specs=vmem,
            scratch_shapes=[
                pltpu.VMEM((layers * mine, patches, chans), BF16),
                pltpu.VMEM(b_tok1.shape, F32),
                pltpu.VMEM(b_tok2.shape, F32),
                pltpu.VMEM(b_ch1.shape, F32),
                pltpu.VMEM(b_ch2.shape, F32),
                pltpu.VMEM(ln_params.shape, F32),
                pltpu.VMEM((layers, tok_hidden, patches), BF16),
                pltpu.VMEM((layers, patches, tok_hidden), BF16),
                pltpu.VMEM((patches, tok_hidden), BF16),
                pltpu.VMEM((tok_hidden, patches), BF16),
                pltpu.VMEM((layers, chans, ch_hidden), BF16),
                pltpu.VMEM((layers, ch_hidden, chans), BF16),
                pltpu.VMEM((patches, chans), BF16),
                pltpu.VMEM((blk, chans), BF16),
                pltpu.VMEM((tok_hidden, chans), BF16),
                pltpu.VMEM((blk, chans), F32),
                [pltpu.VMEM((blk, ECHUNK), BF16)] * 2,
                pltpu.VMEM((layers, tok_hidden, 128), F32),
                pltpu.VMEM((layers, patches, 128), F32),
                dma((mine,)),
                dma((mine, 2)),
                dma((mine,)),
                dma((mine, 2)),
                dma((2,)),
                dma((2, layers)),
                dma((5,)),
            ],
            compiler_params=pltpu.CompilerParams(collective_id=0, has_side_effects=True, vmem_limit_bytes=62783488),
            cost_estimate=pl.CostEstimate(flops=flops, bytes_accessed=2 * x_blk.size * 2, transcendentals=0),
        )(x_blk, w_tok1, b_tok1, w_tok2, b_tok2, w_ch1, b_ch1, w_ch2, b_ch2, ln_params)

    act_spec = P("data", "seq", None)
    rep_spec = P()
    return jax.shard_map(local_layers, mesh=mesh, in_specs=(act_spec,) + (rep_spec,) * 9, out_specs=act_spec, check_vma=False)
```

```python
import functools

import jax
import jax.numpy as jnp
from jax import lax
from jax.experimental import pallas as pl
from jax.experimental.pallas import tpu as pltpu
from jax.sharding import PartitionSpec as P

LN_EPS = 1e-6
GELU_A = 0.7978845608028654
GELU_B = GELU_A * 0.044715
MESH = pl.DeviceIdType.MESH
BF16 = jnp.bfloat16
F32 = jnp.float32
LN_ROWS = 16
UNROLL = 16
SENDS = 8
ECHUNK = 1024


def gelu_twice(h):
    return h + h * jnp.tanh(h * (2 * GELU_A + 8 * GELU_B * (h * h)))


def norm_rows(rows, gamma, beta):
    mean = jnp.mean(rows, axis=-1, keepdims=True)
    cent = rows - mean
    var = jnp.mean(cent * cent, axis=-1, keepdims=True)
    return (cent * lax.rsqrt(var + LN_EPS) * gamma + beta).astype(BF16)


def mixer_kernel(
    n, x_ref, wt1_ref, bt1_hbm, wt2_ref, bt2_hbm, wc1_ref, bc1_hbm, wc2_ref, bc2_hbm, ln_hbm,
    out_ref, state, bt1_ref, bt2_ref, bc1_ref, bc2_ref, ln_ref, w1t, w2t, s1, s2, wc1, wc2, ub, vb, gb, acc, ab, b1c, b2c,
    in_send, in_recv, mid_send, mid_recv, tok_sem, ch_sem, small_sem,
):
    me = lax.axis_index("seq")
    images, rows, chans = x_ref.shape
    mine = images // n
    layers, patches, tok_hidden = wt1_ref.shape
    ch_hidden = wc1_ref.shape[2]
    halves = 2
    blk = patches // halves
    per_blk = n // halves
    echunk = ab[0].shape[1]
    nchunk = ch_hidden // echunk
    my_parity = me // 2 + me // 8
    my_place = (me // 4) * 2 + lax.rem(me, 2)

    def peer_at(b, place):
        pair = place // 2
        return pair * 4 + lax.rem(my_parity + b + pair // 2, 2) * 2 + lax.rem(place, 2)

    def turn(i):
        return lax.rem(my_place + i * 3, per_blk)

    def stage(k):
        return pltpu.make_async_copy(wt1_ref.at[k], s1, tok_sem.at[0]), pltpu.make_async_copy(wt2_ref.at[k], s2, tok_sem.at[1])

    smalls = [
        pltpu.make_async_copy(src, dst, small_sem.at[i])
        for i, (src, dst) in enumerate(
            ((bt1_hbm, bt1_ref), (bt2_hbm, bt2_ref), (bc1_hbm, bc1_ref), (bc2_hbm, bc2_ref), (ln_hbm, ln_ref))
        )
    ]

    barrier = pltpu.get_barrier_semaphore()

    def signal_peer(i, carry):
        pl.semaphore_signal(barrier, inc=1, device_id={"seq": lax.rem(me + i, n)}, device_id_type=MESH)
        return carry

    lax.fori_loop(1, n, signal_peer, 0, unroll=SENDS)

    for copy in (*stage(0), *smalls):
        copy.start()
    pl.semaphore_wait(barrier, n - 1)

    def send_in(img):
        for b in range(halves):
            def one(i, carry, b=b):
                peer = peer_at(b, turn(i))
                pltpu.make_async_remote_copy(
                    src_ref=x_ref.at[peer * mine + img],
                    dst_ref=state.at[img, pl.ds(me * rows, rows)],
                    send_sem=in_send.at[img],
                    recv_sem=in_recv.at[img, b],
                    device_id={"seq": peer},
                    device_id_type=MESH,
                ).start()
                return carry

            if b == 0:
                pltpu.make_async_copy(x_ref.at[me * mine + img], state.at[img, pl.ds(me * rows, rows)], in_recv.at[img, b]).start()
            lax.fori_loop(1 if b == 0 else 0, per_blk, one, 0, unroll=SENDS)

    send_in(0)

    def load_channel(k):
        pltpu.make_async_copy(wc1_ref.at[k], wc1.at[k], ch_sem.at[0, k]).start()
        pltpu.make_async_copy(wc2_ref.at[k], wc2.at[k], ch_sem.at[1, k]).start()

    load_channel(0)

    for copy in smalls:
        copy.wait()
    tile = 256

    def flip(k, carry):
        for copy in stage(k):
            copy.wait()
        for r in range(0, patches, tile):
            w1t[k, :, r : r + tile] = s1[r : r + tile, :].T
        for r in range(0, tok_hidden, tile):
            w2t[k, :, r : r + tile] = s2[r : r + tile, :].T

        @pl.when(k + 1 < layers)
        def _():
            for copy in stage(k + 1):
                copy.start()

        b1c[k] = jnp.broadcast_to(0.5 * bt1_ref[pl.ds(k, 1), :], (128, tok_hidden)).T
        b2c[k] = jnp.broadcast_to(bt2_ref[pl.ds(k, 1), :], (128, patches)).T
        return carry

    lax.fori_loop(0, layers, flip, 0)

    def send_mid(img):
        for b in range(halves):
            def one(i, carry, b=b):
                peer = peer_at(b, turn(i))
                pltpu.make_async_remote_copy(
                    src_ref=state.at[img, pl.ds(peer * rows, rows)],
                    dst_ref=state.at[mine + img, pl.ds(b * blk + my_place * rows, rows)],
                    send_sem=mid_send.at[img],
                    recv_sem=mid_recv.at[img, b],
                    device_id={"seq": peer},
                    device_id_type=MESH,
                ).start()
                return carry

            if b == 0:
                state[mine + img, pl.ds(pl.multiple_of(my_place * rows, rows), rows), :] = state[img, pl.ds(pl.multiple_of(me * rows, rows), rows), :]
            lax.fori_loop(1 if b == 0 else 0, per_blk, one, 0, unroll=SENDS)

    def arrived(slot, b, sem, count):
        at = state.at[slot, pl.ds(b * blk, count * rows)]
        pltpu.make_async_copy(at, at, sem).wait()

    def norm_at(dst, to, slot, start, k, which):
        vals = state[slot, pl.ds(start, LN_ROWS), :].astype(F32)
        dst[pl.ds(to, LN_ROWS), :] = norm_rows(vals, 0.5 * ln_ref[k, pl.ds(which, 1), :], 0.5 * ln_ref[k, pl.ds(which + 1, 1), :])

    def norm_block(dst, to, slot, start, k, which, count):
        def some(r, c):
            off = pl.multiple_of(r * LN_ROWS, LN_ROWS)
            norm_at(dst, to + off, slot, start + off, k, which)
            return c

        lax.fori_loop(0, count // LN_ROWS, some, 0, unroll=UNROLL)

    def token_mix(slot, k, then=None):
        half = chans // 2
        for c in range(0, chans, half):
            h = jnp.dot(w1t[k], ub[:, c : c + half], preferred_element_type=F32) + b1c[k, :, 0:1]
            gb[:, c : c + half] = gelu_twice(h).astype(BF16)
        for r in range(0, patches, blk):
            at = slice(r, r + blk)
            t = (jnp.dot(w2t[k, at, :], gb[...], preferred_element_type=F32) + b2c[k, at, 0:1]).astype(BF16)
            state[slot, at, :] = (state[slot, at, :].astype(F32) + t.astype(F32)).astype(BF16)
            if r == 0 and then is not None:
                then()

    def channel_mlp(slot, k, b):
        lo = pl.multiple_of(b * blk, blk)
        other = jnp.where((slot == mine * layers - 1) | (b == 1), 0, 1) * blk
        side_k = jnp.minimum(k + b, layers - 1)
        side_which = 2 * (1 - b)
        side_rows = blk // nchunk

        def side(e):
            for r in range(e * side_rows, (e + 1) * side_rows, LN_ROWS):
                norm_at(ub, r, slot, pl.multiple_of(other, blk) + r, side_k, side_which)

        def up(e):
            cols = slice(e * echunk, (e + 1) * echunk)
            h = jnp.dot(vb[...], wc1[k, :, cols], preferred_element_type=F32) + 0.5 * bc1_ref[pl.ds(k, 1), cols]
            ab[e % 2][...] = gelu_twice(h).astype(BF16)

        def down(e):
            base = state[slot, pl.ds(lo, blk), :].astype(F32) + bc2_ref[pl.ds(k, 1), :] if e == 0 else acc[...]
            return base + jnp.dot(ab[e % 2][...], wc2[k, e * echunk : (e + 1) * echunk, :], preferred_element_type=F32)

        up(0)
        side(0)
        for e in range(1, nchunk):
            up(e)
            side(e)
            acc[...] = down(e - 1)
        state[slot, pl.ds(lo, blk), :] = down(nchunk - 1).astype(BF16)

    def slot_step(slot, carry):
        k = slot // mine

        @pl.when(slot < mine)
        def _():
            for b in range(halves):
                arrived(slot, b, in_recv.at[slot, b], per_blk)

                if b == 0:
                    @pl.when(slot + 1 < mine)
                    def _():
                        send_in(slot + 1)

                def ln1(i, c, b=b):
                    start = pl.multiple_of(peer_at(b, i) * rows, rows)
                    for r in range(0, rows, LN_ROWS):
                        norm_at(ub, start + r, slot, start + r, 0, 0)
                    return c

                lax.fori_loop(0, per_blk, ln1, 0, unroll=min(UNROLL, per_blk))

            def first_norm():
                for r in range(0, blk, LN_ROWS):
                    norm_at(vb, r, slot, r, 0, 2)

            token_mix(slot, 0, first_norm)

        @pl.when(lax.rem(slot, mine) == 0)
        def _():
            pltpu.make_async_copy(wc1_ref.at[k], wc1.at[k], ch_sem.at[0, k]).wait()
            pltpu.make_async_copy(wc2_ref.at[k], wc2.at[k], ch_sem.at[1, k]).wait()

            @pl.when(k + 1 < layers)
            def _():
                load_channel(k + 1)

        last = mine * layers - 1

        def block(b, c0):
            fresh = (slot >= mine) & ((b == 0) | (slot == last))

            @pl.when((slot >= mine) & (b == 0))
            def _():
                arrived(slot, 0, mid_recv.at[slot - mine, 0], per_blk - 1)

            @pl.when((slot >= mine) & ((b == 1) == (slot == last)))
            def _():
                arrived(slot, 1, mid_recv.at[slot - mine, 1], per_blk)

            @pl.when(fresh)
            def _():
                norm_block(vb, 0, slot, pl.multiple_of(b * blk, blk), k, 2, blk)

            @pl.when((b == 1) & (slot != last))
            def _():
                vb[...] = ub[0:blk, :]

            channel_mlp(slot, k, b)

            @pl.when(slot >= mine)
            def _():
                def one(place, c):
                    at = pl.ds(pl.multiple_of(b * blk + place * rows, rows), rows)
                    out_ref[peer_at(b, place) * mine + slot - mine] = state[slot, at, :]
                    return c

                lax.fori_loop(0, per_blk, one, 0, unroll=4)

            return c0

        lax.fori_loop(0, halves, block, 0)

        @pl.when(slot < mine)
        def _():
            for r in range(blk, patches, LN_ROWS):
                norm_at(ub, r, slot, r, 1, 0)
            token_mix(slot, 1)
            send_mid(slot)

        return carry

    lax.fori_loop(0, mine * layers, slot_step, 0)

    sent = x_ref.at[pl.ds(0, n - 1)]
    for img in range(mine):
        pltpu.make_async_copy(sent, sent, in_send.at[img]).wait()
        pltpu.make_async_copy(sent, sent, mid_send.at[img]).wait()


def solution(mesh):
    n = mesh.shape["seq"]

    def local_layers(x_blk, w_tok1, b_tok1, w_tok2, b_tok2, w_ch1, b_ch1, w_ch2, b_ch2, ln_params):
        images, rows, chans = x_blk.shape
        mine = images // n
        layers, patches, tok_hidden = w_tok1.shape
        ch_hidden = w_ch1.shape[2]
        blk = patches // 2
        hbm = pl.BlockSpec(memory_space=pl.ANY)
        vmem = pl.BlockSpec(memory_space=pltpu.VMEM)
        flops = 4 * mine * layers * patches * chans * (tok_hidden + ch_hidden)
        dma = pltpu.SemaphoreType.DMA
        return pl.pallas_call(
            functools.partial(mixer_kernel, n),
            out_shape=pltpu.VMEM(x_blk.shape, x_blk.dtype),
            in_specs=[hbm] * 10,
            out_specs=vmem,
            scratch_shapes=[
                pltpu.VMEM((layers * mine, patches, chans), BF16),
                pltpu.VMEM(b_tok1.shape, F32),
                pltpu.VMEM(b_tok2.shape, F32),
                pltpu.VMEM(b_ch1.shape, F32),
                pltpu.VMEM(b_ch2.shape, F32),
                pltpu.VMEM(ln_params.shape, F32),
                pltpu.VMEM((layers, tok_hidden, patches), BF16),
                pltpu.VMEM((layers, patches, tok_hidden), BF16),
                pltpu.VMEM((patches, tok_hidden), BF16),
                pltpu.VMEM((tok_hidden, patches), BF16),
                pltpu.VMEM((layers, chans, ch_hidden), BF16),
                pltpu.VMEM((layers, ch_hidden, chans), BF16),
                pltpu.VMEM((patches, chans), BF16),
                pltpu.VMEM((blk, chans), BF16),
                pltpu.VMEM((tok_hidden, chans), BF16),
                pltpu.VMEM((blk, chans), F32),
                [pltpu.VMEM((blk, ECHUNK), BF16)] * 2,
                pltpu.VMEM((layers, tok_hidden, 128), F32),
                pltpu.VMEM((layers, patches, 128), F32),
                dma((mine,)),
                dma((mine, 2)),
                dma((mine,)),
                dma((mine, 2)),
                dma((2,)),
                dma((2, layers)),
                dma((5,)),
            ],
            compiler_params=pltpu.CompilerParams(collective_id=0, has_side_effects=True, vmem_limit_bytes=62783488),
            cost_estimate=pl.CostEstimate(flops=flops, bytes_accessed=2 * x_blk.size * 2, transcendentals=0),
        )(x_blk, w_tok1, b_tok1, w_tok2, b_tok2, w_ch1, b_ch1, w_ch2, b_ch2, ln_params)

    act_spec = P("data", "seq", None)
    rep_spec = P()
    return jax.shard_map(local_layers, mesh=mesh, in_specs=(act_spec,) + (rep_spec,) * 9, out_specs=act_spec, check_vma=False)
```
